512 devices in a mesh: seq: 128 (over x, z, y_hi, core), head: 4 (over y_lo).
Axes of the slice: x: 4, y: 8 (y_hi: 2, y_lo: 4; y = y_hi * 4 + y_lo), z: 8, core: 2. Of those that a mesh axis runs over, the one named last changes fastest.
Arguments:
- queries: bfloat16 [65536, 4096], P('seq', 'head'), may hold values from -72 to 72
- key_heads: bfloat16 [65536, 4096], P('seq', 'head'), may hold values from -6 to 6
- value_heads: bfloat16 [65536, 4096], P('seq', 'head'), may hold values from -6 to 6
- dilation: int32 [4], replicated, may hold values from 1 to 8, as said below
- window: int32 [4], replicated, may hold values from 96 to 192, as said below
Outputs:
- attended: bfloat16 [65536, 4096], P('seq', 'head')
The draws below stay inside these ranges and needn't reach their ends.
Inputs may be any that keep to these rules, and one draw needn't show every extreme that they name: dilation holds the four numbers 1, 2, 4, 8, each once. Each window lies between 96 and 192; the group whose dilation is 8 has exactly 192.
All inputs are finite; a program needn't handle non-finite values.
Results may differ from the reference program's by a relative error of at most 0.0043.
Values may be sent and summed in bfloat16 or wider, within the bound.
A program may use at most 64 MiB of HBM per device.

```python
from functools import partial
import jax
import jax.numpy as jnp
from jax import lax

HEADS = 32
HS = 128
WIN = 192
GROUPS = 4
TOKENS = 65536


def group_draw(key):
    levels = jax.random.permutation(jax.random.fold_in(key, 11), GROUPS).astype(jnp.int32)
    dilation = jnp.left_shift(jnp.ones((GROUPS,), jnp.int32), levels)
    spans = jax.random.randint(jax.random.fold_in(key, 12), (GROUPS,), WIN // 2, WIN + 1, dtype=jnp.int32)
    spans = jnp.where(dilation == 8, WIN, spans).astype(jnp.int32)
    return (dilation, spans)


def draw_dilation(key, part):
    return group_draw(key)[0]


def draw_window(key, part):
    return group_draw(key)[1]


def key_draw(key):
    return jnp.clip(jax.random.normal(jax.random.fold_in(key, 21), (TOKENS, HEADS * HS), jnp.float32), -6.0, 6.0)


def draw_key_heads(key, part):
    return key_draw(key).astype(jnp.bfloat16)


def draw_queries(key, part):
    mixed = jnp.clip(jax.random.normal(jax.random.fold_in(key, 22), (TOKENS, HEADS * HS), jnp.float32), -6.0, 6.0)
    return mixed.astype(jnp.bfloat16)


def shard_levels(stream_key, dims, cuts, low, largest):
    factor_of, own = 1.0, jax.random.fold_in(stream_key, 6)
    for dim, shards_of in cuts:
        draws = jnp.exp(jax.random.uniform(jax.random.fold_in(own, dim), (shards_of,), jnp.float32, low / len(cuts), largest / len(cuts)))
        factor_of = factor_of * jnp.repeat(draws, dims[dim] // shards_of).reshape([-1 if axis == dim else 1 for axis in range(len(dims))])
    return factor_of


def noise(key, dims, scale, reach, cuts=(), kind=jnp.bfloat16):
    gain = shard_levels(key, dims, cuts, -0.22, 0.18) if cuts else 1.0
    result = jax.random.normal(key, dims, jnp.float32) * scale * gain
    return jnp.minimum(jnp.maximum(result, -reach), reach).astype(kind)


def setup_inputs(seed: int = 0) -> dict:
    keys = jax.random.split(jax.random.key(seed), 6)
    queries = draw_queries(jax.random.fold_in(keys[5], 71), 0)
    key_heads = draw_key_heads(jax.random.fold_in(keys[5], 71), 0)
    value_heads = noise(keys[2], (TOKENS, HEADS * HS), 1.0, 6.0, ((0, 128), (1, 4)))
    dilation = draw_dilation(jax.random.fold_in(keys[5], 71), 0)
    window = draw_window(jax.random.fold_in(keys[5], 71), 0)
    return dict(queries=queries, key_heads=key_heads, value_heads=value_heads, dilation=dilation, window=window)


masked_fill = -1.0e30


def group_attend(queries, key_heads, value_heads, reach_keys, degree):
    stride = 2 ** degree
    length, width = queries.shape
    heads_here = width // HS
    padding = jnp.zeros((stride * WIN, width), key_heads.dtype)
    keys_full = jnp.concatenate([padding, key_heads], axis=0)
    values_full = jnp.concatenate([padding, value_heads], axis=0)
    block_rows = min(512, length)
    per_class = block_rows // stride
    class_length = length // stride
    q_split = queries.reshape(class_length, stride, heads_here, HS)
    k_split = keys_full.reshape(class_length + WIN, stride, heads_here, HS)
    v_split = values_full.reshape(class_length + WIN, stride, heads_here, HS)
    scale = HS ** -0.5

    def one_block(number):
        opening = (number * per_class).astype(jnp.int32)
        q_block = lax.dynamic_slice_in_dim(q_split, opening, per_class, 0).astype(jnp.float32)
        k_block = lax.dynamic_slice_in_dim(k_split, opening, per_class + WIN, 0).astype(jnp.float32)
        v_block = lax.dynamic_slice_in_dim(v_split, opening, per_class + WIN, 0).astype(jnp.float32)
        scores = jnp.einsum("urhs,vrhs->rhuv", q_block, k_block) * scale
        query_index = jnp.arange(per_class, dtype=jnp.int32)[:, None]
        key_index = jnp.arange(per_class + WIN, dtype=jnp.int32)[None, :]
        distance = query_index - key_index + WIN
        inside = (distance >= 0) & (distance < reach_keys)
        position = -stride * WIN + (opening + key_index) * stride + jnp.arange(stride, dtype=jnp.int32)[:, None]
        valid = inside[None, None, :, :] & (position >= 0)[:, None, None, :]
        masked = jnp.where(valid, scores, masked_fill)
        peak = jnp.max(masked, axis=-1, keepdims=True)
        weights = jnp.where(valid, jnp.exp(masked - peak), 0.0)
        denominator = jnp.sum(weights, axis=-1)
        rounded = weights.astype(jnp.bfloat16)
        mixed = jnp.einsum("rhuv,vrhs->urhs", rounded.astype(jnp.float32), v_block)
        mixed = mixed / jnp.transpose(denominator, (2, 0, 1))[..., None]
        return mixed.astype(jnp.bfloat16).reshape(block_rows, width)

    blocks_out = lax.map(one_block, jnp.arange(length // block_rows, dtype=jnp.int32))
    return blocks_out.reshape(length, width)


def reference(queries, key_heads, value_heads, dilation, window):
    width = queries.shape[1]
    portion = width // GROUPS
    results = []
    for member in range(GROUPS):
        lower = member * portion
        upper = lower + portion
        level_index = ((dilation[member] > 1).astype(jnp.int32) + (dilation[member] > 2).astype(jnp.int32) + (dilation[member] > 4).astype(jnp.int32))
        branches = [partial(group_attend, degree=degree) for degree in range(4)]
        results.append(lax.switch(level_index, branches, queries[:, lower:upper], key_heads[:, lower:upper], value_heads[:, lower:upper], window[member]))
    return jnp.concatenate(results, axis=1)
```

```python
import itertools
import math
from functools import partial

import jax
import jax.numpy as jnp
from jax import lax
from jax.experimental import pallas as pl
from jax.experimental.pallas import tpu as pltpu
from jax.sharding import PartitionSpec as P

HS = 128
WIN = 192
BLK = 64
MESH = pl.DeviceIdType.MESH
XS, ZS, YS = 4, 8, 8
FACTOR = HS**-0.5 * math.log2(math.e)
FILL = -1e30

ROWS = ((0, 0, 256, 512), (192, 384, 512, 512))


def pick(index, values):
    result = jnp.int32(values[0])
    for i in range(1, len(values)):
        result = jnp.where(index == i, jnp.int32(values[i]), result)
    return result


def place(x, z, y, c):
    return (((x * ZS + z) * 2 + y // 4) * 2 + c, y % 4)


def kernel(
    lev,
    window_ref,
    q_hbm,
    k_hbm,
    v_hbm,
    out_hbm,
    hk,
    hv,
    rv,
    qs,
    ks,
    vs,
    pm,
    pt,
    kp,
    vp,
    qp,
    op,
    ost,
    load_sem,
    out_sem,
    ak_s,
    ak_r,
    bv_s,
    bv_r,
    cv_s,
    cv_r,
    d_s,
    d_r,
    e_s,
    e_r,
    f_s,
    f_r,
):
    length, width = qs.shape
    heads = width // HS
    seat = lax.axis_index("seq")
    g = lax.axis_index("head")
    c = seat % 2
    y = ((seat // 2) % 2) * 4 + g
    z = (seat // 4) % ZS
    x = seat // (4 * ZS)
    level = pick(g, lev)
    relay_level = pick((g + 2) % 4, lev)
    zn = (z + 1) % ZS
    xn = jnp.where(z == ZS - 1, (x + 1) % XS, x)
    zb = (z + ZS - 1) % ZS
    xb = jnp.where(z == 0, (x + XS - 1) % XS, x)
    yo = (y + 4) % 8
    low = y < 4
    step = jnp.where(y % 2 == 0, 2, YS - 2)
    back = YS - step
    xd = jnp.where(low, x, xn)
    zd = jnp.where(low, z, zn)
    to_next = place(xd, zd, yo, c)
    to_relay = place(xd, zd, (y + back) % 8, c)
    rs_y = (y + step) % 8
    rs = place(jnp.where(rs_y < 4, x, xb), jnp.where(rs_y < 4, z, zb), rs_y, c)
    rd = place(x, z, (y + back) % 8, c)
    from_prev = place(jnp.where(low, xb, x), jnp.where(low, zb, z), yo, c)
    from_relay = place(x, z, (yo + back) % 8, c)
    partner = place(x, z, y, 1 - c)
    z_next = place(xn, zn, y, 0)
    z_prev = place(xb, zb, y, 1)

    loads = [
        pltpu.make_async_copy(src, dst, load_sem.at[i])
        for i, (src, dst) in enumerate(((q_hbm, qs), (k_hbm, ks), (v_hbm, vs)))
    ]
    for load in loads:
        load.start()

    for buf in (hk, hv):
        buf[2, 0:320, :] = jnp.zeros((320, width), jnp.bfloat16)
        buf[1, 0:256, :] = jnp.zeros((256, width), jnp.bfloat16)

    barrier = pltpu.get_barrier_semaphore()
    for target in (from_prev, rs, from_relay, partner):
        pl.semaphore_signal(barrier, inc=1, device_id=target, device_id_type=MESH)

    @pl.when(c == 0)
    def _():
        pl.semaphore_signal(barrier, inc=1, device_id=z_prev, device_id_type=MESH)

    span = pick(level, (64, 128, 256, 512))
    dil = pick(level, (1, 2, 4, 8))

    def class_source(i):
        base = i & -span
        return base + (i & (BLK - 1)) * dil + ((i - base) >> 6)

    rows_i = lax.broadcasted_iota(jnp.int32, (length, length), 0)
    cols_i = lax.broadcasted_iota(jnp.int32, (length, length), 1)
    pm[...] = (cols_i == class_source(rows_i)).astype(jnp.float32).astype(jnp.bfloat16)
    pt[...] = (rows_i == class_source(cols_i)).astype(jnp.float32).astype(jnp.bfloat16)

    @pl.when(c == 0)
    def _():
        pl.semaphore_wait(barrier, 4)

    @pl.when(c == 1)
    def _():
        pl.semaphore_wait(barrier, 5)

    own_rows = jnp.where(c == 0, pick(level, ROWS[0]), pick(level, ROWS[1]))
    relay_rows = jnp.where(c == 0, pick(relay_level, ROWS[0]), pick(relay_level, ROWS[1]))

    def sized(rows, fn):
        for size in (192, 256, 384, 512):

            @pl.when(rows == size)
            def _():
                fn(size)

    def cols(h):
        return pl.ds(pl.multiple_of(h * HS, HS), HS)

    def remote(src, dst, send, recv, target):
        return pltpu.make_async_remote_copy(
            src_ref=src, dst_ref=dst, send_sem=send, recv_sem=recv, device_id=target, device_id_type=MESH
        )

    def tail(size):
        return pl.ds(length - size, size)

    def copy_a(size, h):
        return remote(
            k_hbm.at[tail(size), cols(h)], hk.at[1, tail(size), cols(h)], ak_s.at[h], ak_r.at[h], to_next
        )

    def copy_b(size, h):
        return remote(
            v_hbm.at[tail(size), cols(h)], rv.at[tail(size), cols(h)], bv_s.at[h], bv_r.at[h], to_relay
        )

    def copy_c(size, h):
        return remote(
            rv.at[tail(size), cols(h)], hv.at[1, tail(size), cols(h)], cv_s.at[h], cv_r.at[h], rd
        )

    def copy_d(size, h, buf, i):
        return remote(
            buf.at[1, tail(size), cols(h)],
            buf.at[2 * c, tail(size), cols(h)],
            d_s.at[i, h],
            d_r.at[i, h],
            partner,
        )

    def copy_e(size, i):
        src, dst = ((k_hbm, hk), (v_hbm, hv))[i]
        return remote(src.at[tail(size), :], dst.at[2, tail(size), :], e_s.at[i], e_r.at[i], partner)

    def copy_f(h, i):
        src, dst = ((k_hbm, hk), (v_hbm, hv))[i]
        return remote(src.at[:, cols(h)], dst.at[0, :, cols(h)], f_s.at[i, h], f_r.at[i, h], z_next)

    def send_own(size):
        def one(h, carry):
            copy_a(size, h).start()
            copy_b(size, h).start()
            return carry

        lax.fori_loop(0, heads, one, 0)

    sized(own_rows, send_own)

    e_rows = pick(level, ROWS[1])

    @pl.when(c == 0)
    def _():
        def send_e(size):
            copy_e(size, 0).start()
            copy_e(size, 1).start()

        sized(e_rows, send_e)

    @pl.when((c == 1) & (level == 3))
    def _():
        def one(h, carry):
            copy_f(h, 0).start()
            copy_f(h, 1).start()
            return carry

        lax.fori_loop(0, heads, one, 0)

    for load in loads:
        load.wait()

    window = window_ref[g]
    row_u = lax.broadcasted_iota(jnp.int32, (BLK, 4 * BLK), 0)
    key_i = lax.broadcasted_iota(jnp.int32, (BLK, 4 * BLK), 1)
    inside = (key_i <= row_u + WIN) & (key_i > row_u + WIN - window)
    opening = (seat * length) >> level

    def permuted(x_ref):
        return jnp.dot(pm[...], x_ref, preferred_element_type=jnp.float32).astype(jnp.bfloat16)

    def fill(block, k_raw, v_raw):
        both = jnp.concatenate([k_raw, v_raw], axis=1)
        both = permuted(both)
        kp[pl.ds(block, 8)] = both[:, :HS].reshape(8, BLK, HS)
        vp[pl.ds(block, 8)] = both[:, HS:].reshape(8, BLK, HS)

    def duty(h):
        def forward(size):
            copy_b(size, h).wait_recv()
            copy_c(size, h).start()

        sized(relay_rows, forward)

        def share(size):
            copy_a(size, h).wait_recv()
            copy_c(size, h).wait_recv()
            if size == 256:
                return

            @pl.when((c == 1) | (level == 3))
            def _():
                copy_d(size, h, hk, 0).start()
                copy_d(size, h, hv, 1).start()

        sized(own_rows, share)

    def compute(h):
        def landed(size):
            copy_d(size, h, hk, 0).wait_recv()
            copy_d(size, h, hv, 1).wait_recv()

        @pl.when(c == 0)
        def _():
            sized(e_rows, landed)

            @pl.when(level == 3)
            def _():
                copy_f(h, 0).wait_recv()
                copy_f(h, 1).wait_recv()

        @pl.when(c == 1)
        def _():
            @pl.when(h == 0)
            def _():
                def first(size):
                    copy_e(size, 0).wait_recv()
                    copy_e(size, 1).wait_recv()

                sized(e_rows, first)

            @pl.when(level == 3)
            def _():
                landed(512)

        fill(24, ks[:, cols(h)], vs[:, cols(h)])
        fill(16, hk[2, :, cols(h)], hv[2, :, cols(h)])

        @pl.when(level >= 2)
        def _():
            fill(8, hk[1, :, cols(h)], hv[1, :, cols(h)])

        @pl.when(level == 3)
        def _():
            fill(0, hk[0, :, cols(h)], hv[0, :, cols(h)])

        qp[...] = permuted(qs[:, cols(h)]).reshape(8, BLK, HS)
        for b in range(8):
            at = [24 + b - dil * (3 - j) for j in range(4)]
            keys = jnp.concatenate([kp[i] for i in at], axis=0)
            values = jnp.concatenate([vp[i] for i in at], axis=0)
            score = lax.dot_general(
                qp[b], keys, (((1,), (1,)), ((), ())), preferred_element_type=jnp.float32
            )
            first_key = WIN - opening - BLK * (b >> level)
            score = jnp.where(inside & (key_i >= first_key), score, FILL)
            peak = jnp.max(score, axis=1, keepdims=True)
            weight = jnp.exp2((score - peak) * FACTOR)
            total = jnp.sum(weight, axis=1, keepdims=True)
            mixed = jnp.dot(
                weight.astype(jnp.bfloat16), values, preferred_element_type=jnp.float32
            )
            op[b * BLK : (b + 1) * BLK, :] = (mixed / total).astype(jnp.bfloat16)
        ost[:, cols(h)] = jnp.dot(
            pt[...], op[...], preferred_element_type=jnp.float32
        ).astype(jnp.bfloat16)
        pltpu.make_async_copy(ost.at[:, cols(h)], out_hbm.at[:, cols(h)], out_sem.at[h]).start()

    def turn(h, carry):
        @pl.when(h < heads)
        def _():
            duty(h)

        @pl.when(h > 0)
        def _():
            compute(h - 1)

        return carry

    lax.fori_loop(0, heads + 1, turn, 0)

    def finish(h, carry):
        pltpu.make_async_copy(ost.at[:, cols(h)], out_hbm.at[:, cols(h)], out_sem.at[h]).wait()

        def done_own(size):
            copy_a(size, h).wait_send()
            copy_b(size, h).wait_send()
            if size == 256:
                return

            @pl.when((c == 1) | (level == 3))
            def _():
                copy_d(size, h, hk, 0).wait_send()
                copy_d(size, h, hv, 1).wait_send()

        sized(own_rows, done_own)
        sized(relay_rows, lambda size: copy_c(size, h).wait_send())

        @pl.when((c == 1) & (level == 3))
        def _():
            copy_f(h, 0).wait_send()
            copy_f(h, 1).wait_send()

        return carry

    lax.fori_loop(0, heads, finish, 0)

    @pl.when(c == 0)
    def _():
        def done_e(size):
            copy_e(size, 0).wait_send()
            copy_e(size, 1).wait_send()

        sized(e_rows, done_e)


def attend(number, lev, queries, keys, values, window):
    length, width = queries.shape
    heads = width // HS
    anywhere = pl.BlockSpec(memory_space=pl.ANY)
    bf = jnp.bfloat16
    dma = pltpu.SemaphoreType.DMA
    return pl.pallas_call(
        partial(kernel, lev),
        name="attend",
        out_shape=jax.ShapeDtypeStruct((length, width), bf),
        in_specs=[pl.BlockSpec(memory_space=pltpu.SMEM)] + [anywhere] * 3,
        out_specs=anywhere,
        scratch_shapes=[
            pltpu.VMEM((3, length, width), bf),
            pltpu.VMEM((3, length, width), bf),
            pltpu.VMEM((length, width), bf),
            pltpu.VMEM((length, width), bf),
            pltpu.VMEM((length, width), bf),
            pltpu.VMEM((length, width), bf),
            pltpu.VMEM((length, length), bf),
            pltpu.VMEM((length, length), bf),
            pltpu.VMEM((32, BLK, HS), bf),
            pltpu.VMEM((32, BLK, HS), bf),
            pltpu.VMEM((8, BLK, HS), bf),
            pltpu.VMEM((length, HS), bf),
            pltpu.VMEM((length, width), bf),
            dma((3,)),
            dma((heads,)),
        ]
        + [dma((heads,))] * 6
        + [dma((2, heads))] * 2
        + [dma((2,))] * 2
        + [dma((2, heads))] * 2,
        compiler_params=pltpu.CompilerParams(collective_id=number, has_side_effects=True),
    )(window, queries, keys, values)


ORDERS = tuple(itertools.permutations(range(4)))


def body(queries, keys, values, dilation, window):
    levels = (dilation > 1).astype(jnp.int32) + (dilation > 2) + (dilation > 4)
    code = levels[0] * 16 + levels[1] * 4 + levels[2]
    number = jnp.int32(0)
    for i, lev in enumerate(ORDERS):
        number = jnp.where(code == lev[0] * 16 + lev[1] * 4 + lev[2], jnp.int32(i), number)
    branches = [partial(attend, i, lev) for i, lev in enumerate(ORDERS)]
    return lax.switch(number, branches, queries, keys, values, window)


def solution(mesh):
    return jax.shard_map(
        body,
        mesh=mesh,
        in_specs=(P("seq", "head"), P("seq", "head"), P("seq", "head"), P(), P()),
        out_specs=P("seq", "head"),
        check_vma=False,
    )
```

```python
import itertools
import math
from functools import partial

import jax
import jax.numpy as jnp
from jax import lax
from jax.experimental import pallas as pl
from jax.experimental.pallas import tpu as pltpu
from jax.sharding import PartitionSpec as P

HS = 128
WIN = 192
BLK = 64
UNITS = 4
MESH = pl.DeviceIdType.MESH
XS, ZS, YS = 4, 8, 8
FACTOR = HS**-0.5 * math.log2(math.e)
FILL = -1e30

TURNED = (6, 5, 0)

ROWS = ((0, 0, 256, 512), (192, 384, 512, 512))


def pick(index, values):
    result = jnp.int32(values[0])
    for i in range(1, len(values)):
        result = jnp.where(index == i, jnp.int32(values[i]), result)
    return result


def place(x, z, y, c):
    return (((x * ZS + z) * 2 + y // 4) * 2 + c, y % 4)


def kernel(
    lev,
    window_ref,
    q_hbm,
    k_hbm,
    v_hbm,
    out_hbm,
    hk,
    hv,
    rv,
    pm,
    pt,
    kp,
    vp,
    op,
    sc,
    wt,
    ost,
    load_sem,
    out_sem,
    k_s,
    k_r,
    v_s,
    v_r,
    b_r,
    c_s,
    d_s,
    d_r,
    e_s,
    e_r,
    f_s,
    f_r,
):
    length, width = q_hbm.shape
    heads = width // HS
    turned = TURNED[lev[(lev.index(3) + 2) % 4]]
    if turned == 0 and lev.index(3) in (0, 3):
        turned = 3
    seat = lax.axis_index("seq")
    g = lax.axis_index("head")
    c = seat % 2
    y = ((seat // 2) % 2) * 4 + g
    z = (seat // 4) % ZS
    x = seat // (4 * ZS)
    level = pick(g, lev)
    far = level == 3
    relay = pick((g + 2) % 4, lev) == 3
    zn = (z + 1) % ZS
    xn = jnp.where(z == ZS - 1, (x + 1) % XS, x)
    zb = (z + ZS - 1) % ZS
    xb = jnp.where(z == 0, (x + XS - 1) % XS, x)
    yo = (y + 4) % 8
    step = jnp.where(y % 2 == 0, 2, YS - 2)
    back = YS - step
    up_y = (y + step) % 8
    down_y = (y + back) % 8

    def after(source_y, target_y):
        return place(jnp.where(source_y < 4, x, xn), jnp.where(source_y < 4, z, zn), target_y, c)

    def before(source_y):
        return place(jnp.where(source_y < 4, x, xb), jnp.where(source_y < 4, z, zb), source_y, c)

    to_next = after(y, yo)
    from_prev = before(yo)
    partner = place(x, z, y, 1 - c)
    z_next = place(xn, zn, y, 0)
    z_prev = place(xb, zb, y, 1)
    to_relay = after(y, down_y)
    source = before(up_y)
    target = place(x, z, down_y, c)

    barrier = pltpu.get_barrier_semaphore()

    def tell(condition, target):
        @pl.when(condition)
        def _():
            pl.semaphore_signal(barrier, inc=1, device_id=target, device_id_type=MESH)

    pl.semaphore_signal(barrier, inc=1, device_id=from_prev, device_id_type=MESH)
    tell(relay, source)
    tell(far, place(x, z, (yo + back) % 8, c))
    tell(far & (c == 0), z_prev)
    pl.semaphore_signal(barrier, inc=1, device_id=partner, device_id_type=MESH)

    loads = [
        pltpu.make_async_copy(src, dst, load_sem.at[i])
        for i, (src, dst) in enumerate(((q_hbm, hk.at[4]), (k_hbm, hk.at[3]), (v_hbm, hv.at[3])))
    ]
    for load in loads:
        load.start()

    def clear(slot, blocks):
        def one(i, carry):
            for buf in (hk, hv):
                buf[slot, pl.ds(i * 16, 16), :] = jnp.zeros((16, width), jnp.bfloat16)
            return carry

        lax.fori_loop(0, blocks, one, 0)

    clear(jnp.where(level == 2, 1, 2), jnp.where((level == 2) & (c == 0), 16, pick(level, (20, 8, 0, 0))))

    span = pick(level, (64, 128, 256, 512))
    dil = pick(level, (1, 2, 4, 8))

    def class_source(i):
        base = i & -span
        return base + (i & (BLK - 1)) * dil + ((i - base) >> 6)

    def build(i, carry):
        rows = pl.ds(i * 16, 16)
        r = lax.broadcasted_iota(jnp.int32, (16, length), 0) + i * 16
        k = lax.broadcasted_iota(jnp.int32, (16, length), 1)
        pm[rows, :] = (k == class_source(r)).astype(jnp.float32).astype(jnp.bfloat16)
        pt[rows, :] = (r == class_source(k)).astype(jnp.float32).astype(jnp.bfloat16)
        return carry

    lax.fori_loop(0, length // 16, build, 0)

    pl.semaphore_wait(
        barrier, 2 + jnp.where(far | relay, 1, 0) + jnp.where(far & (c == 1), 1, 0)
    )

    own_rows = jnp.where(c == 0, pick(level, ROWS[0]), pick(level, ROWS[1]))

    def sized(rows, fn, sizes=(192, 256, 384, 512)):
        for size in sizes:

            @pl.when(rows == size)
            def _():
                fn(size)

    def cols(h):
        return pl.ds(pl.multiple_of(h * HS, HS), HS)

    def remote(src, dst, send, recv, target):
        return pltpu.make_async_remote_copy(
            src_ref=src, dst_ref=dst, send_sem=send, recv_sem=recv, device_id=target, device_id_type=MESH
        )

    def tail(size):
        return pl.ds(length - size, size)

    def copy_k(size, h):
        return remote(
            k_hbm.at[tail(size), cols(h)], hk.at[1, tail(size), cols(h)], k_s.at[h], k_r.at[h], to_next
        )

    def copy_v(size, h):
        return remote(
            v_hbm.at[tail(size), cols(h)], hv.at[1, tail(size), cols(h)], v_s.at[h], v_r.at[h], to_next
        )

    def copy_b(h):
        return remote(v_hbm.at[:, cols(h)], rv.at[:, cols(h)], v_s.at[h], b_r.at[h], to_relay)

    def copy_c(h):
        return remote(rv.at[:, cols(h)], hv.at[1, :, cols(h)], c_s.at[h], v_r.at[h], target)

    def copy_d(size, h, buf, i):
        return remote(
            buf.at[1, tail(size), cols(h)],
            buf.at[2 * c, tail(size), cols(h)],
            d_s.at[i, h],
            d_r.at[i, h],
            partner,
        )

    def copy_e(size, i):
        src, dst = ((k_hbm, hk), (v_hbm, hv))[i]
        return remote(src.at[tail(size), :], dst.at[2, tail(size), :], e_s.at[i], e_r.at[i], partner)

    def copy_f(h, i):
        src, dst = ((k_hbm, hk), (v_hbm, hv))[i]
        return remote(src.at[:, cols(h)], dst.at[0, :, cols(h)], f_s.at[i, h], f_r.at[i, h], z_next)

    def every_head(fn):
        def one(h, carry):
            fn(h)
            return carry

        lax.fori_loop(0, heads, one, 0)

    @pl.when(far)
    def _():
        def one(h, carry):
            copy_b(h).start()
            return carry

        lax.fori_loop(turned, heads, one, 0)

    def send_head(size, h):
        copy_k(size, h).start()
        if size < 512:
            copy_v(size, h).start()
            return

        @pl.when(jnp.logical_not(far & (h >= turned)))
        def _():
            copy_v(size, h).start()

    sized(own_rows, lambda size: every_head(lambda h: send_head(size, h)))

    e_rows = pick(level, ROWS[1])

    @pl.when(far & (c == 1))
    def _():
        def one(h):
            copy_f(h, 0).start()
            copy_f(h, 1).start()

        every_head(one)

    @pl.when(c == 0)
    def _():
        def send_e(size):
            copy_e(size, 0).start()
            copy_e(size, 1).start()

        sized(e_rows, send_e, ROWS[1][:3])

    for load in loads:
        load.wait()

    window = window_ref[g]
    row_u = lax.broadcasted_iota(jnp.int32, (BLK, 4 * BLK), 0)
    key_i = lax.broadcasted_iota(jnp.int32, (BLK, 4 * BLK), 1)
    inside = (key_i <= row_u + WIN) & (key_i > row_u + WIN - window)
    opening = (seat * length) >> level
    slots = pick(level, (2, 2, 1, 0))

    def duty(h):
        @pl.when(relay & (h + turned < heads))
        def _():
            copy_b(h + turned).wait_recv()
            copy_c(h + turned).start()

        def share(size):
            copy_k(size, h).wait_recv()
            copy_v(size, h).wait_recv()
            if size == 256:
                return

            @pl.when((c == 1) | far)
            def _():
                copy_d(size, h, hk, 0).start()
                copy_d(size, h, hv, 1).start()

        sized(own_rows, share)

    def landed(size, h):
        copy_d(size, h, hk, 0).wait_recv()
        copy_d(size, h, hv, 1).wait_recv()

    def arrive(h):
        @pl.when(c == 0)
        def _():
            sized(e_rows, lambda size: landed(size, h), ROWS[1][:3])

            @pl.when(far)
            def _():
                copy_f(h, 0).wait_recv()
                copy_f(h, 1).wait_recv()

        @pl.when((c == 1) & far)
        def _():
            landed(512, h)

    @pl.when(c == 1)
    def _():
        def first(size):
            copy_e(size, 0).wait_recv()
            copy_e(size, 1).wait_recv()

        sized(e_rows, first, ROWS[1][:3])

    def turn(t, carry):
        before_loop = t < heads
        h = jnp.where(before_loop, t, t - heads - 1)

        @pl.when((t >= heads) & (t < 2 * heads))
        def _():
            duty(t - heads)

        @pl.when(t > heads)
        def _():
            arrive(h)

        def fill(s, carry):
            both = jnp.concatenate([hk[s, :, cols(h)], hv[s, :, cols(h)]], axis=1)
            both = jnp.dot(pm[...], both, preferred_element_type=jnp.float32).astype(jnp.bfloat16)
            kp[h, pl.ds(8 * s, 8)] = both[:, :HS].reshape(8, BLK, HS)
            vp[h, pl.ds(8 * s, 8)] = both[:, HS:].reshape(8, BLK, HS)
            return carry

        lax.fori_loop(
            jnp.where(before_loop, 3 - c, slots),
            jnp.where(before_loop, 5, jnp.where(t == heads, 0, 3 - c)),
            fill,
            0,
        )

        @pl.when(t > heads)
        def _():
            compute(h)

        return carry

    def compute(h):
        def units(half, carry):
            blocks = [half * UNITS + i for i in range(UNITS)]
            for i, b in enumerate(blocks):
                keys = jnp.concatenate([kp[h, 24 + b - dil * (3 - j)] for j in range(4)], axis=0)
                sc[i] = lax.dot_general(
                    kp[h, 32 + b], keys, (((1,), (1,)), ((), ())), preferred_element_type=jnp.float32
                )
            totals = []
            for i, b in enumerate(blocks):
                first_key = WIN - opening - BLK * (b >> level)
                score = jnp.where(inside & (key_i >= first_key), sc[i], FILL)
                peak = jnp.max(score, axis=1, keepdims=True)
                weight = jnp.exp2((score - peak) * FACTOR)
                totals.append(jnp.sum(weight, axis=1, keepdims=True))
                wt[i] = weight.astype(jnp.bfloat16)
            for i, b in enumerate(blocks):
                values = jnp.concatenate([vp[h, 24 + b - dil * (3 - j)] for j in range(4)], axis=0)
                mixed = jnp.dot(wt[i], values, preferred_element_type=jnp.float32)
                op[b] = (mixed / totals[i]).astype(jnp.bfloat16)
            return carry

        lax.fori_loop(0, 8 // UNITS, units, 0)

        def restore(i, carry):
            rows = pl.ds(pl.multiple_of(i * (length // 2), length // 2), length // 2)
            ost[rows, cols(h)] = jnp.dot(
                pt[rows, :], op[...].reshape(length, HS), preferred_element_type=jnp.float32
            ).astype(jnp.bfloat16)
            return carry

        lax.fori_loop(0, 2, restore, 0)
        pltpu.make_async_copy(ost.at[:, cols(h)], out_hbm.at[:, cols(h)], out_sem.at[h]).start()

    lax.fori_loop(0, 2 * heads + 1, turn, 0)

    def finish(h):
        pltpu.make_async_copy(ost.at[:, cols(h)], out_hbm.at[:, cols(h)], out_sem.at[h]).wait()

        def done_own(size):
            copy_k(size, h).wait_send()
            copy_v(size, h).wait_send()
            if size == 256:
                return

            @pl.when((c == 1) | far)
            def _():
                copy_d(size, h, hk, 0).wait_send()
                copy_d(size, h, hv, 1).wait_send()

        sized(own_rows, done_own)

        @pl.when(relay & (h >= turned))
        def _():
            copy_c(h).wait_send()

        @pl.when(far & (c == 1))
        def _():
            copy_f(h, 0).wait_send()
            copy_f(h, 1).wait_send()

    every_head(finish)

    @pl.when(c == 0)
    def _():
        def done_e(size):
            copy_e(size, 0).wait_send()
            copy_e(size, 1).wait_send()

        sized(e_rows, done_e, ROWS[1][:3])


def attend(number, lev, queries, keys, values, window):
    length, width = queries.shape
    heads = width // HS
    anywhere = pl.BlockSpec(memory_space=pl.ANY)
    bf = jnp.bfloat16
    dma = pltpu.SemaphoreType.DMA
    return pl.pallas_call(
        partial(kernel, lev),
        name="attend",
        out_shape=jax.ShapeDtypeStruct((length, width), bf),
        in_specs=[pl.BlockSpec(memory_space=pltpu.SMEM)] + [anywhere] * 3,
        out_specs=anywhere,
        scratch_shapes=[
            pltpu.VMEM((5, length, width), bf),
            pltpu.VMEM((5, length, width), bf),
            pltpu.VMEM((length, width), bf),
            pltpu.VMEM((length, length), bf),
            pltpu.VMEM((length, length), bf),
            pltpu.VMEM((heads, 40, BLK, HS), bf),
            pltpu.VMEM((heads, 40, BLK, HS), bf),
            pltpu.VMEM((8, BLK, HS), bf),
            pltpu.VMEM((UNITS, BLK, 4 * BLK), jnp.float32),
            pltpu.VMEM((UNITS, BLK, 4 * BLK), bf),
            pltpu.VMEM((length, width), bf),
            dma((3,)),
        ]
        + [dma((heads,))] * 7
        + [dma((2, heads))] * 2
        + [dma((2,))] * 2
        + [dma((2, heads))] * 2,
        compiler_params=pltpu.CompilerParams(collective_id=number, has_side_effects=True),
    )(window, queries, keys, values)


ORDERS = tuple(itertools.permutations(range(4)))


def body(queries, keys, values, dilation, window):
    levels = (dilation > 1).astype(jnp.int32) + (dilation > 2) + (dilation > 4)
    code = levels[0] * 16 + levels[1] * 4 + levels[2]
    number = jnp.int32(0)
    for i, lev in enumerate(ORDERS):
        number = jnp.where(code == lev[0] * 16 + lev[1] * 4 + lev[2], jnp.int32(i), number)
    branches = [partial(attend, i, lev) for i, lev in enumerate(ORDERS)]
    return lax.switch(number, branches, queries, keys, values, window)


def solution(mesh):
    return jax.shard_map(
        body,
        mesh=mesh,
        in_specs=(P("seq", "head"), P("seq", "head"), P("seq", "head"), P(), P()),
        out_specs=P("seq", "head"),
        check_vma=False,
    )
```
